32 devices in a mesh: row: 8 (over z, core), col: 4 (over y, x).
Axes of the slice: x: 2, y: 2, z: 4, core: 2. Of those that a mesh axis runs over, the one named last changes fastest.
Arguments:
- tokens: bfloat16 [16384, 6144], P(('row', 'col')), may hold values from -6 to 6
- grad_out: bfloat16 [16384, 6144], P(('row', 'col')), may hold values from -6 to 6
- w_up: bfloat16 [6144, 512], replicated, may hold values from -0.078125 to 0.078125
- w_down: bfloat16 [512, 6144], replicated, may hold values from -0.0390625 to 0.0390625
Outputs:
- up_grad: float32 [6144, 512], P('row', 'col')
- down_grad: float32 [6144, 512], P('row', 'col')
The draws below stay inside these ranges and needn't reach their ends.
All inputs are finite; a program needn't handle non-finite values.
Results may differ from the reference program's by a relative error of at most 0.0041.
Values may be sent and summed in bfloat16 or wider, within the bound.
A program may use at most 128 MiB of HBM per device.

```python
import math
import jax
import jax.numpy as jnp
from jax import lax

D = 6144
FF = 24576
C = 512
TOK_DEV = 512
TOKENS = 16384
N_ROW = 8
N_COL = 4


def shard_levels(own_key, shape, cuts, least, top_value):
    factor_of, own = 1.0, jax.random.fold_in(own_key, 6)
    for dim, blocks in cuts:
        steps = jnp.exp(jax.random.uniform(jax.random.fold_in(own, dim), (blocks,), jnp.float32, least / len(cuts), top_value / len(cuts)))
        factor_of = factor_of * jnp.repeat(steps, shape[dim] // blocks).reshape([-1 if axis == dim else 1 for axis in range(len(shape))])
    return factor_of


def normal_values(stream_key, dims, spread, most, cuts=(), kind=jnp.bfloat16):
    drawn = jax.random.normal(stream_key, dims, jnp.float32) * spread
    if len(cuts) > 0:
        drawn = shard_levels(stream_key, dims, cuts, -0.22, 0.18) * drawn
    return jnp.clip(drawn, min=-most, max=most).astype(kind)


def setup_inputs(seed: int = 0) -> dict:
    streams_of = jax.random.split(jax.random.key(seed), 5)
    tokens = normal_values(streams_of[0], (TOKENS, D), 1.0, 6.0, ((0, 32),))
    grad_out = normal_values(streams_of[1], (TOKENS, D), 1.0, 6.0, ((0, 32),))
    w_up = normal_values(streams_of[2], (D, C), D ** -0.5, 0.078125)
    w_down = normal_values(streams_of[3], (C, D), FF ** -0.5, 0.0390625)
    return {"tokens": tokens, "grad_out": grad_out, "w_up": w_up, "w_down": w_down}


def gelu_parts(preact):
    cumul = 0.5 * (1.0 + jax.scipy.special.erf(preact / math.sqrt(2.0)))
    density = jnp.exp(-0.5 * preact * preact) / math.sqrt(2.0 * math.pi)
    return (preact * cumul, cumul + preact * density)

def rounded(term):
    levels = term.astype(jnp.bfloat16)
    levels = lax.optimization_barrier(levels)
    return levels.astype(jnp.float32)

def reference(tokens, grad_out, w_up, w_down):

    def one_device(totals, index):
        start = (index * TOK_DEV).astype(jnp.int32)
        own_tok = lax.dynamic_slice_in_dim(tokens, start, TOK_DEV, 0)
        own_grad = lax.dynamic_slice_in_dim(grad_out, start, TOK_DEV, 0)
        preact = jnp.dot(own_tok, w_up, preferred_element_type=jnp.float32)
        act_grad = jnp.dot(own_grad, w_down.T, preferred_element_type=jnp.float32)
        value, slope = gelu_parts(preact)
        act = value.astype(jnp.bfloat16)
        hidden_grad = (act_grad * slope).astype(jnp.bfloat16)
        term_up = jnp.dot(own_tok.T, hidden_grad, preferred_element_type=jnp.float32)
        term_down = jnp.dot(own_grad.T, act, preferred_element_type=jnp.float32)
        return ((totals[0] + rounded(term_up), totals[1] + rounded(term_down)), None)
    zeros = jnp.zeros((D, C), jnp.float32)
    count = N_ROW * N_COL
    (sum_up, sum_down), _ = lax.scan(one_device, (zeros, zeros), jnp.arange(count, dtype=jnp.int32))
    factor = 1.0 / math.sqrt(TOKENS)
    return (sum_up * factor, sum_down * factor)
```

```python
import functools
import math

import jax
import jax.numpy as jnp
from jax import lax
from jax.experimental import pallas as pl
from jax.experimental.pallas import tpu as pltpu
from jax.sharding import PartitionSpec as P

MESH = pl.DeviceIdType.MESH
F32 = jnp.float32
BF16 = jnp.bfloat16


def gelu_parts(preact):
    cumul = 0.5 * (1.0 + lax.erf(preact * (1.0 / math.sqrt(2.0))))
    density = jnp.exp(-0.5 * preact * preact) * (1.0 / math.sqrt(2.0 * math.pi))
    return (preact * cumul, cumul + preact * density)


def kernel(A, B, Z, tok_hbm, grad_hbm, wup_hbm, wdn_hbm, out_down, out_up,
           wide, oth, wu, wd, acc, acc2, slope, lhs, term,
           r1d, r1u, q2d, q2u, r2d, r2u, q3, r3,
           ld, cs, cr, ls, lr, s1d, s1u, g1d, g1u, s2d, s2u, g2d, g2u, s3, g3):
    T, D = tok_hbm.shape
    C = wup_hbm.shape[1]
    db = D // (2 * Z)
    cb = C // (A * B)
    nt = 256 if db % 256 == 0 else 128
    row, col = lax.axis_index("row"), lax.axis_index("col")
    core, z = lax.rem(row, 2), row // 2
    a, b = lax.rem(col, A), col // A

    def at(b_, a_):
        return (row, b_ * A + a_)

    peer = (z * 2 + (1 - core), col)

    def cols(k, c):
        return pl.ds(pl.multiple_of((2 * k + c) * db, db), db)

    def load_first(k):
        return [
            pltpu.make_async_copy(tok_hbm.at[:, cols(k, core)], wide.at[1, k, pl.ds(0, T)], ld.at[0, k]),
            pltpu.make_async_copy(wup_hbm.at[cols(k, core)], wu.at[k, 0], ld.at[1, k]),
            pltpu.make_async_copy(tok_hbm.at[:, cols(k, 1 - core)], oth.at[1, k], ld.at[2, k]),
            pltpu.make_async_copy(wup_hbm.at[cols(k, 1 - core)], wu.at[k, 1], ld.at[3, k]),
        ]

    def load_second(k):
        return [
            pltpu.make_async_copy(grad_hbm.at[:, cols(k, core)], wide.at[0, k, pl.ds(0, T)], ld.at[4, k]),
            pltpu.make_async_copy(wdn_hbm.at[:, cols(k, core)], wd.at[k, 0], ld.at[5, k]),
            pltpu.make_async_copy(grad_hbm.at[:, cols(k, 1 - core)], oth.at[0, k], ld.at[6, k]),
            pltpu.make_async_copy(wdn_hbm.at[:, cols(k, 1 - core)], wd.at[k, 1], ld.at[7, k]),
        ]

    for k in range(Z):
        for copy in load_first(k):
            copy.start()

    barrier = pltpu.get_barrier_semaphore()
    partners = [peer]
    partners += [at(b, lax.rem(a + d, A)) for d in range(1, A)]
    partners += [at(lax.rem(b + d, B), a) for d in range(1, B)]
    partners += [(lax.rem(z + d, Z) * 2 + core, col) for d in range(1, Z)]
    for partner in partners:
        pl.semaphore_signal(barrier, inc=1, device_id=partner, device_id_type=MESH)
    pl.semaphore_wait(barrier, len(partners))

    def swap(bucket, k):
        source = (grad_hbm, tok_hbm)[bucket]
        return pltpu.make_async_remote_copy(
            source.at[:, cols(k, 1 - core)], wide.at[bucket, k, pl.ds(T, T)],
            cs.at[bucket, k], cr.at[bucket, k], device_id=peer, device_id_type=MESH)

    def swap_lhs(bucket):
        return pltpu.make_async_remote_copy(
            lhs.at[bucket, :, pl.ds(0, T)], lhs.at[bucket, :, pl.ds(T, T)],
            ls.at[bucket], lr.at[bucket], device_id=peer, device_id_type=MESH)

    def block(t):
        return lax.rem(z + 1 + t, Z)

    for t in range(Z):
        swap(0, block(t)).start()
    for k in range(Z):
        for copy in load_second(k):
            copy.start()
    for t in range(Z):
        swap(1, block(t)).start()

    acc[...] = jnp.zeros_like(acc)

    def preact_step(k, carry):
        for copy in load_first(k):
            copy.wait()
        acc[...] += (jnp.dot(wide[1, k, :T], wu[k, 0], preferred_element_type=F32)
                     + jnp.dot(oth[1, k], wu[k, 1], preferred_element_type=F32))
        return carry

    lax.fori_loop(0, Z, preact_step, 0)

    def gelu_step(i, carry):
        part = pl.ds(pl.multiple_of(i * 128, 128), 128)
        value, steep = gelu_parts(acc[:, part].T)
        lhs[0, part, :T] = value.astype(BF16)
        slope[part, :] = steep
        return carry

    lax.fori_loop(0, C // 128, gelu_step, 0)
    swap_lhs(0).start()

    acc2[...] = jnp.zeros_like(acc2)
    across = (((1,), (1,)), ((), ()))

    def grad_step(k, carry):
        for copy in load_second(k):
            copy.wait()
        acc2[...] += (lax.dot_general(wd[k, 0], wide[0, k, :T], across, preferred_element_type=F32)
                      + lax.dot_general(wd[k, 1], oth[0, k], across, preferred_element_type=F32))
        return carry

    lax.fori_loop(0, Z, grad_step, 0)
    lhs[1, :, :T] = (acc2[...] * slope[...]).astype(BF16)
    swap_lhs(1).start()

    def send1(bucket, t):
        if bucket == 0:
            return [pltpu.make_async_remote_copy(
                term.at[0, t, lax.rem(b + d, B)], r1d.at[t, d - 1], s1d.at[t, d - 1], g1d.at[t, d - 1],
                device_id=at(lax.rem(b + d, B), a), device_id_type=MESH) for d in range(1, B)]
        return [pltpu.make_async_remote_copy(
            term.at[1, t, :, lax.rem(a + d, A)], r1u.at[t, d - 1], s1u.at[t, d - 1], g1u.at[t, d - 1],
            device_id=at(b, lax.rem(a + d, A)), device_id_type=MESH) for d in range(1, A)]

    def send2(bucket, t):
        if bucket == 0:
            return [pltpu.make_async_remote_copy(
                q2d.at[t, d - 1], r2d.at[t, d - 1], s2d.at[t, d - 1], g2d.at[t, d - 1],
                device_id=at(b, lax.rem(a + d, A)), device_id_type=MESH) for d in range(1, A)]
        return [pltpu.make_async_remote_copy(
            q2u.at[t, d - 1], r2u.at[t, d - 1], s2u.at[t, d - 1], g2u.at[t, d - 1],
            device_id=at(lax.rem(b + d, B), a), device_id_type=MESH) for d in range(1, B)]

    def send3(bucket, t):
        return pltpu.make_async_remote_copy(
            q3.at[bucket, t], r3.at[bucket, t], s3.at[bucket, t], g3.at[bucket, t],
            device_id=(block(t) * 2 + core, col), device_id_type=MESH)

    def sum1(bucket, t, b_, a_):
        total = term[bucket, t, b_, a_].astype(F32)
        if bucket == 0:
            for d in range(B - 1):
                total += r1d[t, d, a_].astype(F32)
        else:
            for d in range(A - 1):
                total += r1u[t, d, b_].astype(F32)
        return total

    def sum2(bucket, t):
        total = sum1(bucket, t, b, a)
        got, count = ((r2d, A - 1), (r2u, B - 1))[bucket]
        for d in range(count):
            total += got[t, d].astype(F32)
        return total

    def start1(t):
        for bucket in range(2):
            for copy in send1(bucket, t):
                copy.start()

    def term_step(t, carry):
        k = block(t)
        for bucket in range(2):
            swap(bucket, k).wait_recv()

            @pl.when(t == 0)
            def _():
                swap_lhs(bucket).wait_recv()

            for n in range(0, db, nt):
                out = jnp.dot(lhs[bucket], wide[bucket, k, :, n:n + nt], preferred_element_type=F32)
                term[bucket, t, :, :, :, n:n + nt] = out.astype(BF16).reshape(B, A, cb, nt)

            @pl.when(t < 2)
            def _():
                for copy in send1(bucket, t):
                    copy.start()
        return carry

    lax.fori_loop(0, Z, term_step, 0)

    def finish2(t):
        for bucket in range(2):
            for copy in send2(bucket, t):
                copy.wait_recv()
            if t < Z - 1:
                q3[bucket, t] = sum2(bucket, t).astype(BF16)
                send3(bucket, t).start()

    for t in range(Z):
        for bucket in range(2):
            for copy in send1(bucket, t):
                copy.wait_recv()
            if bucket == 0:
                for d in range(1, A):
                    q2d[t, d - 1] = sum1(0, t, b, lax.rem(a + d, A)).astype(BF16)
            else:
                for d in range(1, B):
                    q2u[t, d - 1] = sum1(1, t, lax.rem(b + d, B), a).astype(BF16)
            for copy in send2(bucket, t):
                copy.start()
        if t + 2 < Z - 1:
            start1(t + 2)
        if t == Z - 2 and Z - 1 >= 2:
            start1(Z - 1)
        if t >= 1:
            finish2(t - 1)
    finish2(Z - 1)

    for bucket, out in enumerate((out_down, out_up)):
        total = sum2(bucket, Z - 1)
        for t in range(Z - 1):
            send3(bucket, t).wait_recv()
            total += r3[bucket, t].astype(F32)
        out[...] = total

    for bucket in range(2):
        swap_lhs(bucket).wait_send()
        for t in range(Z):
            swap(bucket, block(t)).wait_send()
            for copy in send1(bucket, t) + send2(bucket, t):
                copy.wait_send()
            if t < Z - 1:
                send3(bucket, t).wait_send()


def local(A, B, Z, tokens, grad_out, w_up, w_down):
    T, D = tokens.shape
    C = w_up.shape[1]
    db, cb = D // (2 * Z), C // (A * B)
    one = lambda n: max(n, 1)
    dma = lambda *shape: pltpu.SemaphoreType.DMA(shape)
    hop = lambda: [dma(Z, one(B - 1)), dma(Z, one(A - 1))]
    hop2 = lambda: [dma(Z, one(A - 1)), dma(Z, one(B - 1))]
    any_spec = pl.BlockSpec(memory_space=pl.ANY)
    vmem_spec = pl.BlockSpec(memory_space=pltpu.VMEM)
    piece = jax.ShapeDtypeStruct((cb, db), F32)
    down, up = pl.pallas_call(
        functools.partial(kernel, A, B, Z),
        out_shape=(piece, piece),
        in_specs=[any_spec] * 4,
        out_specs=(vmem_spec, vmem_spec),
        scratch_shapes=[
            pltpu.VMEM((2, Z, 2 * T, db), BF16),
            pltpu.VMEM((2, Z, T, db), BF16),
            pltpu.VMEM((Z, 2, db, C), BF16),
            pltpu.VMEM((Z, 2, C, db), BF16),
            pltpu.VMEM((T, C), F32),
            pltpu.VMEM((C, T), F32),
            pltpu.VMEM((C, T), F32),
            pltpu.VMEM((2, C, 2 * T), BF16),
            pltpu.VMEM((2, Z, B, A, cb, db), BF16),
            pltpu.VMEM((Z, one(B - 1), A, cb, db), BF16),
            pltpu.VMEM((Z, one(A - 1), B, cb, db), BF16),
            pltpu.VMEM((Z, one(A - 1), cb, db), BF16),
            pltpu.VMEM((Z, one(B - 1), cb, db), BF16),
            pltpu.VMEM((Z, one(A - 1), cb, db), BF16),
            pltpu.VMEM((Z, one(B - 1), cb, db), BF16),
            pltpu.VMEM((2, one(Z - 1), cb, db), BF16),
            pltpu.VMEM((2, one(Z - 1), cb, db), BF16),
            dma(8, Z), dma(2, Z), dma(2, Z), dma(2), dma(2),
            *hop(), *hop(), *hop2(), *hop2(),
            dma(2, one(Z - 1)), dma(2, one(Z - 1)),
        ],
        compiler_params=pltpu.CompilerParams(
            collective_id=0, has_side_effects=True, vmem_limit_bytes=66000000
        ),
    )(tokens, grad_out, w_up, w_down)
    total_tokens = T * lax.axis_size("row") * lax.axis_size("col")
    factor = 1.0 / math.sqrt(total_tokens)
    return (up.T * factor, down.T * factor)


def solution(mesh):
    rows, columns = mesh.shape["row"], mesh.shape["col"]
    A = 2 if columns % 2 == 0 else 1
    placed = (P(("row", "col"), None), P(("row", "col"), None), P(), P())
    return jax.shard_map(
        functools.partial(local, A, columns // A, rows // 2),
        mesh=mesh,
        in_specs=placed,
        out_specs=(P("row", "col"), P("row", "col")),
        check_vma=False,
    )
```

```python
import functools
import math

import jax
import jax.numpy as jnp
from jax import lax
from jax.experimental import pallas as pl
from jax.experimental.pallas import tpu as pltpu
from jax.sharding import PartitionSpec as P

MESH = pl.DeviceIdType.MESH
F32 = jnp.float32
BF16 = jnp.bfloat16


def gelu_parts(preact):
    cumul = 0.5 * (1.0 + lax.erf(preact * (1.0 / math.sqrt(2.0))))
    density = jnp.exp(-0.5 * preact * preact) * (1.0 / math.sqrt(2.0 * math.pi))
    return (preact * cumul, cumul + preact * density)


def kernel(A, B, Z, tok_hbm, grad_hbm, wup_hbm, wdn_hbm, out_down, out_up,
           wide, oth, wu, wd, acc, acc2, slope, lhs, term,
           r1d, r1u, q2d, q2u, r2d, r2u, q3, r3,
           ld, cs, cr, ls, lr, s1d, s1u, g1d, g1u, s2d, s2u, g2d, g2u, s3, g3):
    T, D = tok_hbm.shape
    C = wup_hbm.shape[1]
    db = D // (2 * Z)
    cb = C // (A * B)
    nt = 256 if db % 256 == 0 else 128
    row, col = lax.axis_index("row"), lax.axis_index("col")
    core, z = lax.rem(row, 2), row // 2
    a, b = lax.rem(col, A), col // A

    def at(b_, a_):
        return (row, b_ * A + a_)

    peer = (z * 2 + (1 - core), col)

    def cols(k, c):
        return pl.ds(pl.multiple_of((2 * k + c) * db, db), db)

    def load_first(k):
        return [
            pltpu.make_async_copy(tok_hbm.at[:, cols(k, core)], wide.at[1, k, pl.ds(0, T)], ld.at[0, k]),
            pltpu.make_async_copy(wup_hbm.at[cols(k, core)], wu.at[k, 0], ld.at[1, k]),
            pltpu.make_async_copy(tok_hbm.at[:, cols(k, 1 - core)], oth.at[1, k], ld.at[2, k]),
            pltpu.make_async_copy(wup_hbm.at[cols(k, 1 - core)], wu.at[k, 1], ld.at[3, k]),
        ]

    def load_second(k):
        return [
            pltpu.make_async_copy(grad_hbm.at[:, cols(k, core)], wide.at[0, k, pl.ds(0, T)], ld.at[4, k]),
            pltpu.make_async_copy(wdn_hbm.at[:, cols(k, core)], wd.at[k, 0], ld.at[5, k]),
            pltpu.make_async_copy(grad_hbm.at[:, cols(k, 1 - core)], oth.at[0, k], ld.at[6, k]),
            pltpu.make_async_copy(wdn_hbm.at[:, cols(k, 1 - core)], wd.at[k, 1], ld.at[7, k]),
        ]

    for k in range(Z):
        for copy in load_first(k):
            copy.start()

    barrier = pltpu.get_barrier_semaphore()
    partners = [peer]
    partners += [at(b, lax.rem(a + d, A)) for d in range(1, A)]
    partners += [at(lax.rem(b + d, B), a) for d in range(1, B)]
    partners += [(lax.rem(z + d, Z) * 2 + core, col) for d in range(1, Z)]
    for partner in partners:
        pl.semaphore_signal(barrier, inc=1, device_id=partner, device_id_type=MESH)
    pl.semaphore_wait(barrier, len(partners))

    def swap(bucket, k):
        source = (grad_hbm, tok_hbm)[bucket]
        return pltpu.make_async_remote_copy(
            source.at[:, cols(k, 1 - core)], wide.at[bucket, k, pl.ds(T, T)],
            cs.at[bucket, k], cr.at[bucket, k], device_id=peer, device_id_type=MESH)

    def swap_lhs(bucket):
        return pltpu.make_async_remote_copy(
            lhs.at[bucket, :, pl.ds(0, T)], lhs.at[bucket, :, pl.ds(T, T)],
            ls.at[bucket], lr.at[bucket], device_id=peer, device_id_type=MESH)

    def block(t):
        return lax.rem(z + 1 + t, Z)

    def chunk(p):
        if p >= 2 * Z - 2:
            return p - (2 * Z - 2), Z - 1
        return p // (Z - 1), p % (Z - 1)

    for t in range(Z):
        swap(0, block(t)).start()
    for k in range(Z):
        for copy in load_second(k):
            copy.start()
    for t in range(Z):
        swap(1, block(t)).start()

    acc[...] = jnp.zeros_like(acc)

    def preact_step(k, carry):
        for copy in load_first(k):
            copy.wait()
        acc[...] += (jnp.dot(wide[1, k, :T], wu[k, 0], preferred_element_type=F32)
                     + jnp.dot(oth[1, k], wu[k, 1], preferred_element_type=F32))
        return carry

    lax.fori_loop(0, Z, preact_step, 0)

    def gelu_step(i, carry):
        part = pl.ds(pl.multiple_of(i * 128, 128), 128)
        value, steep = gelu_parts(acc[:, part].T)
        lhs[0, part, :T] = value.astype(BF16)
        slope[part, :] = steep
        return carry

    lax.fori_loop(0, C // 128, gelu_step, 0)
    swap_lhs(0).start()

    def send1(h, u):
        if h == 0:
            return [pltpu.make_async_remote_copy(
                term.at[2 * u, lax.rem(b + d, B)], r1d.at[u, d - 1], s1d.at[u, d - 1], g1d.at[u, d - 1],
                device_id=at(lax.rem(b + d, B), a), device_id_type=MESH) for d in range(1, B)]
        return [pltpu.make_async_remote_copy(
            term.at[2 * u + 1, :, lax.rem(a + d, A)], r1u.at[u, d - 1], s1u.at[u, d - 1], g1u.at[u, d - 1],
            device_id=at(b, lax.rem(a + d, A)), device_id_type=MESH) for d in range(1, A)]

    def send2(h, u):
        if h == 0:
            return [pltpu.make_async_remote_copy(
                q2d.at[u, d - 1], r2d.at[u, d - 1], s2d.at[u, d - 1], g2d.at[u, d - 1],
                device_id=at(b, lax.rem(a + d, A)), device_id_type=MESH) for d in range(1, A)]
        return [pltpu.make_async_remote_copy(
            q2u.at[u, d - 1], r2u.at[u, d - 1], s2u.at[u, d - 1], g2u.at[u, d - 1],
            device_id=at(lax.rem(b + d, B), a), device_id_type=MESH) for d in range(1, B)]

    def send3(bucket, t):
        return pltpu.make_async_remote_copy(
            q3.at[bucket, t], r3.at[bucket, t], s3.at[bucket, t], g3.at[bucket, t],
            device_id=(block(t) * 2 + core, col), device_id_type=MESH)

    def sum1(h, u, b_, a_):
        total = term[2 * u + h, b_, a_].astype(F32)
        if h == 0:
            for d in range(B - 1):
                total += r1d[u, d, a_].astype(F32)
        else:
            for d in range(A - 1):
                total += r1u[u, d, b_].astype(F32)
        return total

    def sum2(h, u):
        total = sum1(h, u, b, a)
        got, count = ((r2d, A - 1), (r2u, B - 1))[h]
        for d in range(count):
            total += got[u, d].astype(F32)
        return total

    def term_of(bucket):
        swap_lhs(bucket).wait_recv()

        def term_step(t, p):
            k = block(t)
            swap(bucket, k).wait_recv()
            if bucket == 0:
                load_second(k)[0].wait()
            for n in range(0, db, nt):
                out = jnp.dot(lhs[bucket], wide[bucket, k, :, n:n + nt], preferred_element_type=F32)
                term[p, :, :, :, n:n + nt] = out.astype(BF16).reshape(B, A, cb, nt)
            for h in range(2):
                @pl.when((p < 4) & (lax.rem(p, 2) == h))
                def _():
                    for copy in send1(h, p // 2):
                        copy.start()

        def loop_step(t, carry):
            term_step(t, bucket * (Z - 1) + t)
            return carry

        lax.fori_loop(0, Z - 1, loop_step, 0)
        term_step(Z - 1, 2 * Z - 2 + bucket)

    term_of(0)

    acc2[...] = jnp.zeros_like(acc2)
    across = (((1,), (1,)), ((), ()))

    def grad_step(k, carry):
        for copy in load_second(k)[1:]:
            copy.wait()
        acc2[...] += (lax.dot_general(wd[k, 0], wide[0, k, :T], across, preferred_element_type=F32)
                      + lax.dot_general(wd[k, 1], oth[0, k], across, preferred_element_type=F32))
        return carry

    lax.fori_loop(0, Z, grad_step, 0)
    lhs[1, :, :T] = (acc2[...] * slope[...]).astype(BF16)
    swap_lhs(1).start()
    term_of(1)

    def step1(h, u):
        for copy in send1(h, u):
            copy.wait_recv()
        if h == 0:
            for d in range(1, A):
                q2d[u, d - 1] = sum1(0, u, b, lax.rem(a + d, A)).astype(BF16)
        else:
            for d in range(1, B):
                q2u[u, d - 1] = sum1(1, u, lax.rem(b + d, B), a).astype(BF16)
        for copy in send2(h, u):
            copy.start()

    def step2(h, u):
        for copy in send2(h, u):
            copy.wait_recv()
        bucket, t = chunk(2 * u + h)
        if t < Z - 1:
            q3[bucket, t] = sum2(h, u).astype(BF16)
            send3(bucket, t).start()

    def start1(u):
        if 2 <= u < Z:
            for h in range(2):
                for copy in send1(h, u):
                    copy.start()

    for u in range(Z):
        if u >= 1 and u == Z - 1:
            for h in range(2):
                step2(h, u - 1)
        for h in range(2):
            step1(h, u)
        if u + 2 < Z - 1:
            start1(u + 2)
        if u == Z - 2:
            start1(Z - 1)
        if u >= 1 and u < Z - 1:
            for h in range(2):
                step2(h, u - 1)
    for h, out in enumerate((out_down, out_up)):
        step2(h, Z - 1)
        total = sum2(h, Z - 1)
        for t in range(Z - 1):
            send3(h, t).wait_recv()
            total += r3[h, t].astype(F32)
        out[...] = total.T

    for h in range(2):
        swap_lhs(h).wait_send()
        for t in range(Z):
            swap(h, block(t)).wait_send()
            for copy in send1(h, t) + send2(h, t):
                copy.wait_send()
            if t < Z - 1:
                send3(h, t).wait_send()


def local(A, B, Z, tokens, grad_out, w_up, w_down):
    T, D = tokens.shape
    C = w_up.shape[1]
    db, cb = D // (2 * Z), C // (A * B)
    one = lambda n: max(n, 1)
    dma = lambda *shape: pltpu.SemaphoreType.DMA(shape)
    hop = lambda: [dma(Z, one(B - 1)), dma(Z, one(A - 1))]
    hop2 = lambda: [dma(Z, one(A - 1)), dma(Z, one(B - 1))]
    any_spec = pl.BlockSpec(memory_space=pl.ANY)
    vmem_spec = pl.BlockSpec(memory_space=pltpu.VMEM)
    piece = jax.ShapeDtypeStruct((db, cb), F32)
    down, up = pl.pallas_call(
        functools.partial(kernel, A, B, Z),
        out_shape=(piece, piece),
        in_specs=[any_spec] * 4,
        out_specs=(vmem_spec, vmem_spec),
        scratch_shapes=[
            pltpu.VMEM((2, Z, 2 * T, db), BF16),
            pltpu.VMEM((2, Z, T, db), BF16),
            pltpu.VMEM((Z, 2, db, C), BF16),
            pltpu.VMEM((Z, 2, C, db), BF16),
            pltpu.VMEM((T, C), F32),
            pltpu.VMEM((C, T), F32),
            pltpu.VMEM((C, T), F32),
            pltpu.VMEM((2, C, 2 * T), BF16),
            pltpu.VMEM((2 * Z, B, A, cb, db), BF16),
            pltpu.VMEM((Z, one(B - 1), A, cb, db), BF16),
            pltpu.VMEM((Z, one(A - 1), B, cb, db), BF16),
            pltpu.VMEM((Z, one(A - 1), cb, db), BF16),
            pltpu.VMEM((Z, one(B - 1), cb, db), BF16),
            pltpu.VMEM((Z, one(A - 1), cb, db), BF16),
            pltpu.VMEM((Z, one(B - 1), cb, db), BF16),
            pltpu.VMEM((2, one(Z - 1), cb, db), BF16),
            pltpu.VMEM((2, one(Z - 1), cb, db), BF16),
            dma(8, Z), dma(2, Z), dma(2, Z), dma(2), dma(2),
            *hop(), *hop(), *hop2(), *hop2(),
            dma(2, one(Z - 1)), dma(2, one(Z - 1)),
        ],
        compiler_params=pltpu.CompilerParams(
            collective_id=0, has_side_effects=True, vmem_limit_bytes=66000000
        ),
    )(tokens, grad_out, w_up, w_down)
    total_tokens = T * lax.axis_size("row") * lax.axis_size("col")
    factor = 1.0 / math.sqrt(total_tokens)
    return (up * factor, down * factor)


def solution(mesh):
    rows, columns = mesh.shape["row"], mesh.shape["col"]
    A = 2 if columns % 2 == 0 else 1
    placed = (P(("row", "col"), None), P(("row", "col"), None), P(), P())
    return jax.shard_map(
        functools.partial(local, A, columns // A, rows // 2),
        mesh=mesh,
        in_specs=placed,
        out_specs=(P("row", "col"), P("row", "col")),
        check_vma=False,
    )
```

```python
import functools
import math

import jax
import jax.numpy as jnp
from jax import lax
from jax.experimental import pallas as pl
from jax.experimental.pallas import tpu as pltpu
from jax.sharding import PartitionSpec as P

MESH = pl.DeviceIdType.MESH
F32 = jnp.float32
BF16 = jnp.bfloat16


def gelu_parts(preact):
    cumul = 0.5 * (1.0 + lax.erf(preact * (1.0 / math.sqrt(2.0))))
    density = jnp.exp(-0.5 * preact * preact) * (1.0 / math.sqrt(2.0 * math.pi))
    return (preact * cumul, cumul + preact * density)


def kernel(A, B, Z, tok_hbm, grad_hbm, wup_hbm, wdn_hbm, out_down, out_up,
           wide, oth, wu, wd, acc, acc2, slope, lhs, term,
           r1d, r1u, q2d, q2u, r2d, r2u, q3, r3,
           ld, cs, cr, ls, lr, s1d, s1u, g1d, g1u, s2d, s2u, g2d, g2u, s3, g3):
    T, D = tok_hbm.shape
    C = wup_hbm.shape[1]
    db = D // (2 * Z)
    cb = C // (A * B)
    nt = 256 if db % 256 == 0 else 128
    row, col = lax.axis_index("row"), lax.axis_index("col")
    core, z = lax.rem(row, 2), row // 2
    a, b = lax.rem(col, A), col // A

    def at(b_, a_):
        return (row, b_ * A + a_)

    peer = (z * 2 + (1 - core), col)

    def cols(k, c):
        return pl.ds(pl.multiple_of((2 * k + c) * db, db), db)

    def load_first(k):
        return [
            pltpu.make_async_copy(tok_hbm.at[:, cols(k, core)], wide.at[1, k, pl.ds(0, T)], ld.at[0, k]),
            pltpu.make_async_copy(wup_hbm.at[cols(k, core)], wu.at[k, 0], ld.at[1, k]),
            pltpu.make_async_copy(tok_hbm.at[:, cols(k, 1 - core)], oth.at[1, k], ld.at[2, k]),
            pltpu.make_async_copy(wup_hbm.at[cols(k, 1 - core)], wu.at[k, 1], ld.at[3, k]),
        ]

    def load_second(k):
        return [
            pltpu.make_async_copy(grad_hbm.at[:, cols(k, core)], wide.at[0, k, pl.ds(0, T)], ld.at[4, k]),
            pltpu.make_async_copy(wdn_hbm.at[:, cols(k, core)], wd.at[k, 0], ld.at[5, k]),
            pltpu.make_async_copy(grad_hbm.at[:, cols(k, 1 - core)], oth.at[0, k], ld.at[6, k]),
            pltpu.make_async_copy(wdn_hbm.at[:, cols(k, 1 - core)], wd.at[k, 1], ld.at[7, k]),
        ]

    for k in range(Z):
        for copy in load_first(k):
            copy.start()

    for k in range(Z):
        for copy in load_second(k):
            copy.start()

    barrier = pltpu.get_barrier_semaphore()
    partners = [peer]
    partners += [at(b, lax.rem(a + d, A)) for d in range(1, A)]
    partners += [at(lax.rem(b + d, B), a) for d in range(1, B)]
    partners += [(lax.rem(z + d, Z) * 2 + core, col) for d in range(1, Z)]
    for partner in partners:
        pl.semaphore_signal(barrier, inc=1, device_id=partner, device_id_type=MESH)
    pl.semaphore_wait(barrier, len(partners))

    def swap(bucket, k):
        source = (grad_hbm, tok_hbm)[bucket]
        return pltpu.make_async_remote_copy(
            source.at[:, cols(k, 1 - core)], wide.at[bucket, k, pl.ds(T, T)],
            cs.at[bucket, k], cr.at[bucket, k], device_id=peer, device_id_type=MESH)

    def swap_lhs(bucket):
        return pltpu.make_async_remote_copy(
            lhs.at[bucket, :, pl.ds(0, T)], lhs.at[bucket, :, pl.ds(T, T)],
            ls.at[bucket], lr.at[bucket], device_id=peer, device_id_type=MESH)

    def block(t):
        return lax.rem(z + 1 + t, Z)

    def chunk(p):
        if p >= 2 * Z - 2:
            return p - (2 * Z - 2), Z - 1
        return p // (Z - 1), p % (Z - 1)

    for t in range(Z):
        swap(0, block(t)).start()
    for t in range(Z):
        swap(1, block(t)).start()

    acc[...] = jnp.zeros_like(acc)

    def preact_step(k, carry):
        for copy in load_first(k):
            copy.wait()
        acc[...] += (jnp.dot(wide[1, k, :T], wu[k, 0], preferred_element_type=F32)
                     + jnp.dot(oth[1, k], wu[k, 1], preferred_element_type=F32))
        return carry

    lax.fori_loop(0, Z, preact_step, 0)

    def gelu_step(i, carry):
        part = pl.ds(pl.multiple_of(i * 128, 128), 128)
        value, steep = gelu_parts(acc[:, part].T)
        lhs[0, part, :T] = value.astype(BF16)
        slope[part, :] = steep
        return carry

    lax.fori_loop(0, C // 128, gelu_step, 0)
    swap_lhs(0).start()

    def send1(h, u):
        if h == 0:
            return [pltpu.make_async_remote_copy(
                term.at[2 * u, lax.rem(b + d, B)], r1d.at[u, d - 1], s1d.at[u, d - 1], g1d.at[u, d - 1],
                device_id=at(lax.rem(b + d, B), a), device_id_type=MESH) for d in range(1, B)]
        return [pltpu.make_async_remote_copy(
            term.at[2 * u + 1, :, lax.rem(a + d, A)], r1u.at[u, d - 1], s1u.at[u, d - 1], g1u.at[u, d - 1],
            device_id=at(b, lax.rem(a + d, A)), device_id_type=MESH) for d in range(1, A)]

    def send2(h, u):
        if h == 0:
            return [pltpu.make_async_remote_copy(
                q2d.at[u, d - 1], r2d.at[u, d - 1], s2d.at[u, d - 1], g2d.at[u, d - 1],
                device_id=at(b, lax.rem(a + d, A)), device_id_type=MESH) for d in range(1, A)]
        return [pltpu.make_async_remote_copy(
            q2u.at[u, d - 1], r2u.at[u, d - 1], s2u.at[u, d - 1], g2u.at[u, d - 1],
            device_id=at(lax.rem(b + d, B), a), device_id_type=MESH) for d in range(1, B)]

    def send3(bucket, t):
        return pltpu.make_async_remote_copy(
            q3.at[bucket, t], r3.at[bucket, t], s3.at[bucket, t], g3.at[bucket, t],
            device_id=(block(t) * 2 + core, col), device_id_type=MESH)

    def sum1(h, u, b_, a_):
        total = term[2 * u + h, b_, a_].astype(F32)
        if h == 0:
            for d in range(B - 1):
                total += r1d[u, d, a_].astype(F32)
        else:
            for d in range(A - 1):
                total += r1u[u, d, b_].astype(F32)
        return total

    def sum2(h, u):
        total = sum1(h, u, b, a)
        got, count = ((r2d, A - 1), (r2u, B - 1))[h]
        for d in range(count):
            total += got[u, d].astype(F32)
        return total

    def term_of(bucket):
        swap_lhs(bucket).wait_recv()

        def term_step(t, p):
            k = block(t)
            swap(bucket, k).wait_recv()
            if bucket == 0:
                load_second(k)[0].wait()
            for n in range(0, db, nt):
                out = jnp.dot(lhs[bucket], wide[bucket, k, :, n:n + nt], preferred_element_type=F32)
                term[p, :, :, :, n:n + nt] = out.astype(BF16).reshape(B, A, cb, nt)
            for h in range(2):
                @pl.when((p < 4) & (lax.rem(p, 2) == h))
                def _():
                    for copy in send1(h, p // 2):
                        copy.start()

        def loop_step(t, carry):
            term_step(t, bucket * (Z - 1) + t)
            return carry

        lax.fori_loop(0, Z - 1, loop_step, 0)
        term_step(Z - 1, 2 * Z - 2 + bucket)

    term_of(0)

    acc2[...] = jnp.zeros_like(acc2)
    across = (((1,), (1,)), ((), ()))

    def grad_step(k, carry):
        for copy in load_second(k)[1:]:
            copy.wait()
        acc2[...] += (lax.dot_general(wd[k, 0], wide[0, k, :T], across, preferred_element_type=F32)
                      + lax.dot_general(wd[k, 1], oth[0, k], across, preferred_element_type=F32))
        return carry

    lax.fori_loop(0, Z, grad_step, 0)
    lhs[1, :, :T] = (acc2[...] * slope[...]).astype(BF16)
    swap_lhs(1).start()
    term_of(1)

    def step1(h, u):
        for copy in send1(h, u):
            copy.wait_recv()
        if h == 0:
            for d in range(1, A):
                q2d[u, d - 1] = sum1(0, u, b, lax.rem(a + d, A)).astype(BF16)
        else:
            for d in range(1, B):
                q2u[u, d - 1] = sum1(1, u, lax.rem(b + d, B), a).astype(BF16)
        for copy in send2(h, u):
            copy.start()

    def step2(h, u):
        for copy in send2(h, u):
            copy.wait_recv()
        bucket, t = chunk(2 * u + h)
        if t < Z - 1:
            q3[bucket, t] = sum2(h, u).astype(BF16)
            send3(bucket, t).start()

    def start1(u):
        if 2 <= u < Z:
            for h in range(2):
                for copy in send1(h, u):
                    copy.start()

    for u in range(Z):
        if u >= 1 and u == Z - 1:
            for h in range(2):
                step2(h, u - 1)
        for h in range(2):
            step1(h, u)
        if u + 2 < Z - 1:
            start1(u + 2)
        if u == Z - 2:
            start1(Z - 1)
        if u >= 1 and u < Z - 1:
            for h in range(2):
                step2(h, u - 1)
    for h, out in enumerate((out_down, out_up)):
        step2(h, Z - 1)
        total = sum2(h, Z - 1)
        for t in range(Z - 1):
            send3(h, t).wait_recv()
            total += r3[h, t].astype(F32)
        out[...] = total.T

    for h in range(2):
        swap_lhs(h).wait_send()
        for t in range(Z):
            swap(h, block(t)).wait_send()
            for copy in send1(h, t) + send2(h, t):
                copy.wait_send()
            if t < Z - 1:
                send3(h, t).wait_send()


def local(A, B, Z, tokens, grad_out, w_up, w_down):
    T, D = tokens.shape
    C = w_up.shape[1]
    db, cb = D // (2 * Z), C // (A * B)
    one = lambda n: max(n, 1)
    dma = lambda *shape: pltpu.SemaphoreType.DMA(shape)
    hop = lambda: [dma(Z, one(B - 1)), dma(Z, one(A - 1))]
    hop2 = lambda: [dma(Z, one(A - 1)), dma(Z, one(B - 1))]
    any_spec = pl.BlockSpec(memory_space=pl.ANY)
    vmem_spec = pl.BlockSpec(memory_space=pltpu.VMEM)
    piece = jax.ShapeDtypeStruct((db, cb), F32)
    down, up = pl.pallas_call(
        functools.partial(kernel, A, B, Z),
        out_shape=(piece, piece),
        in_specs=[any_spec] * 4,
        out_specs=(vmem_spec, vmem_spec),
        scratch_shapes=[
            pltpu.VMEM((2, Z, 2 * T, db), BF16),
            pltpu.VMEM((2, Z, T, db), BF16),
            pltpu.VMEM((Z, 2, db, C), BF16),
            pltpu.VMEM((Z, 2, C, db), BF16),
            pltpu.VMEM((T, C), F32),
            pltpu.VMEM((C, T), F32),
            pltpu.VMEM((C, T), F32),
            pltpu.VMEM((2, C, 2 * T), BF16),
            pltpu.VMEM((2 * Z, B, A, cb, db), BF16),
            pltpu.VMEM((Z, one(B - 1), A, cb, db), BF16),
            pltpu.VMEM((Z, one(A - 1), B, cb, db), BF16),
            pltpu.VMEM((Z, one(A - 1), cb, db), BF16),
            pltpu.VMEM((Z, one(B - 1), cb, db), BF16),
            pltpu.VMEM((Z, one(A - 1), cb, db), BF16),
            pltpu.VMEM((Z, one(B - 1), cb, db), BF16),
            pltpu.VMEM((2, one(Z - 1), cb, db), BF16),
            pltpu.VMEM((2, one(Z - 1), cb, db), BF16),
            dma(8, Z), dma(2, Z), dma(2, Z), dma(2), dma(2),
            *hop(), *hop(), *hop2(), *hop2(),
            dma(2, one(Z - 1)), dma(2, one(Z - 1)),
        ],
        compiler_params=pltpu.CompilerParams(
            collective_id=0, has_side_effects=True, vmem_limit_bytes=66000000
        ),
    )(tokens, grad_out, w_up, w_down)
    total_tokens = T * lax.axis_size("row") * lax.axis_size("col")
    factor = 1.0 / math.sqrt(total_tokens)
    return (up * factor, down * factor)


def solution(mesh):
    rows, columns = mesh.shape["row"], mesh.shape["col"]
    A = 2 if columns % 2 == 0 else 1
    placed = (P(("row", "col"), None), P(("row", "col"), None), P(), P())
    return jax.shard_map(
        functools.partial(local, A, columns // A, rows // 2),
        mesh=mesh,
        in_specs=placed,
        out_specs=(P("row", "col"), P("row", "col")),
        check_vma=False,
    )
```
